256 devices in a mesh: dp: 16 (over z, core), row: 4 (over y), col: 4 (over x).
Axes of the slice: x: 4, y: 4, z: 8, core: 2. Of those that a mesh axis runs over, the one named last changes fastest.
Arguments:
- grad_up: bfloat16 [16, 2048, 8192], P('dp', 'col', 'row'), may hold values from -24 to 24
- grad_down: bfloat16 [16, 8192, 2048], P('dp', 'row', 'col'), may hold values from -24 to 24
- master_up: float32 [2048, 8192], P('col', ('row', 'dp')), may hold values from -6 to 6
- moment_up: float32 [2048, 8192], P('col', ('row', 'dp')), may hold values from -3 to 3
- second_up: float32 [2048, 8192], P('col', ('row', 'dp')), may hold values from 0.01 to 1
- master_down: float32 [8192, 2048], P(('row', 'dp'), 'col'), may hold values from -6 to 6
- moment_down: float32 [8192, 2048], P(('row', 'dp'), 'col'), may hold values from -3 to 3
- second_down: float32 [8192, 2048], P(('row', 'dp'), 'col'), may hold values from 0.01 to 1
Outputs:
- new_master_up: float32 [2048, 8192], P('col', ('row', 'dp'))
- new_moment_up: float32 [2048, 8192], P('col', ('row', 'dp'))
- new_second_up: float32 [2048, 8192], P('col', ('row', 'dp'))
- new_master_down: float32 [8192, 2048], P(('row', 'dp'), 'col')
- new_moment_down: float32 [8192, 2048], P(('row', 'dp'), 'col')
- new_second_down: float32 [8192, 2048], P(('row', 'dp'), 'col')
- weight_up: bfloat16 [2048, 8192], P('col', 'row')
- weight_down: bfloat16 [8192, 2048], P('row', 'col')
The draws below stay inside these ranges and needn't reach their ends.
All inputs are finite; a program needn't handle non-finite values.
Results may differ from the reference program's by a relative error of at most 0.012.
Values may be sent and summed in bfloat16 or wider, within the bound.
A program may use at most 64 MiB of HBM per device.

```python
import math
import jax
import jax.numpy as jnp
from jax import lax

D = 2048
FF = 8192
STEP = 10
N_DP = 16


def strengthened(entries, own_key, source, target, parts, factor):
    owner, partner = [(jnp.arange(entries.shape[axis_at]) // (entries.shape[axis_at] // parts)).reshape([-1 if axis == axis_at else 1 for axis in range(entries.ndim)]) for axis_at in (source, target)]
    chosen = jax.random.permutation(own_key, parts)[partner]
    strong = (owner == chosen) | (owner == (partner + parts // 2) % parts)
    return jnp.where(strong, factor * entries, entries)


def block_scale(own_key, extent, cuts, smallest, high):
    def one(position, parts):
        draws = jax.random.uniform(jax.random.fold_in(jax.random.fold_in(own_key, 6), position), (parts,), jnp.float32, smallest / len(cuts), high / len(cuts))
        return jnp.repeat(jnp.exp(draws), extent[position] // parts).reshape((-1,) + (1,) * (len(extent) - position - 1))

    factor_of = one(*cuts[0])
    for cut in cuts[1:]:
        factor_of = factor_of * one(*cut)
    return factor_of


def noise(key, shape, deviation, reach, pieces=(), held_as=jnp.bfloat16):
    values = deviation * jax.random.normal(key, shape, jnp.float32)
    if pieces:
        values = values * block_scale(key, shape, pieces, -0.22, 0.18)
    return jnp.clip(values, -reach, reach).astype(held_as)


def noise_with(rng, extent, deviation, limit, pieces, heavy, kind=jnp.bfloat16):
    entries = deviation * jax.random.normal(rng, extent, jnp.float32)
    if pieces:
        entries = entries * block_scale(rng, extent, pieces, -0.22, 0.18)
    return jnp.clip(strengthened(entries, jax.random.fold_in(rng, 3), *heavy), -limit, limit).astype(kind)


def setup_inputs(seed: int = 0) -> dict:
    key_of = jax.random.split(jax.random.key(seed), 9)
    grad_up = noise_with(key_of[0], (N_DP, D, FF), 4.0, 24.0, ((0, 16), (1, 4), (2, 4)), (0, 2, 16, 2.0))
    grad_down = noise_with(key_of[1], (N_DP, FF, D), 4.0, 24.0, ((0, 16), (1, 4), (2, 4)), (0, 1, 16, 2.0))
    master_up = noise(key_of[2], (D, FF), 1.0, 6.0, ((0, 4), (1, 64)), jnp.float32)
    moment_up = noise(key_of[3], (D, FF), 0.5, 3.0, ((0, 4), (1, 64)), jnp.float32)
    second_up = jnp.clip(jnp.exp(math.log(1.0) - 4.6051702 * jax.random.uniform(key_of[4], (D, FF), jnp.float32) ** block_scale(key_of[4], (D, FF), ((0, 4), (1, 64)), -0.2, 0.2)), 0.01, 1.0)
    master_down = noise(key_of[5], (FF, D), 1.0, 6.0, ((0, 64), (1, 4)), jnp.float32)
    moment_down = noise(key_of[6], (FF, D), 0.5, 3.0, ((0, 64), (1, 4)), jnp.float32)
    second_down = jnp.clip(jnp.exp(math.log(1.0) - 4.6051702 * jax.random.uniform(key_of[7], (FF, D), jnp.float32) ** block_scale(key_of[7], (FF, D), ((0, 64), (1, 4)), -0.2, 0.2)), 0.01, 1.0)
    return dict(grad_up=grad_up, grad_down=grad_down, master_up=master_up, moment_up=moment_up, second_up=second_up, master_down=master_down, moment_down=moment_down, second_down=second_down)


def adam_move(master, moment, second, grad):
    new_moment = 0.9 * moment + 0.1 * grad
    new_second = 0.95 * second + 0.05 * grad * grad
    first_hat = new_moment / (1.0 - 0.9 ** STEP)
    second_hat = new_second / (1.0 - 0.95 ** STEP)
    moved = master - 0.2 * first_hat / (jnp.sqrt(second_hat) + 1e-08)
    return (moved, new_moment, new_second)

def reference(grad_up, grad_down, master_up, moment_up, second_up, master_down, moment_down, second_down):
    summed_up = lax.optimization_barrier(jnp.sum(grad_up, axis=0, dtype=jnp.float32)) / N_DP
    summed_down = lax.optimization_barrier(jnp.sum(grad_down, axis=0, dtype=jnp.float32)) / N_DP
    moved_up, mom_up, sec_up = adam_move(master_up, moment_up, second_up, summed_up)
    moved_down, mom_down, sec_down = adam_move(master_down, moment_down, second_down, summed_down)
    norm_up = moved_up * jax.lax.rsqrt(lax.optimization_barrier(jnp.mean(moved_up * moved_up, axis=0, keepdims=True)) + 1e-06)
    norm_down = moved_down * jax.lax.rsqrt(lax.optimization_barrier(jnp.mean(moved_down * moved_down, axis=1, keepdims=True)) + 1e-06)
    return (norm_up, mom_up, sec_up, norm_down, mom_down, sec_down, norm_up.astype(jnp.bfloat16), norm_down.astype(jnp.bfloat16))
```

```python
import jax
import jax.numpy as jnp
from jax import lax
from jax.experimental import pallas as pl
from jax.experimental.pallas import tpu as pltpu
from jax.sharding import PartitionSpec as P

D = 2048
STEP = 10
MESH = pl.DeviceIdType.MESH
F32, BF16 = jnp.float32, jnp.bfloat16
NZ = 8
S = 2
UP, DOWN = 0, 1
RIGHT, LEFT = 0, 1
A, B = 0, 1
BLOCK = ((512, 128), (128, 512))
PIECE = tuple((r // (2 * S), c) for r, c in BLOCK)
OPT = ((512, 128), (128, 512))


def adam_move(master, moment, second, grad):
    new_moment = 0.9 * moment + 0.1 * grad
    new_second = 0.95 * second + 0.05 * grad * grad
    first_hat = new_moment / (1.0 - 0.9**STEP)
    second_hat = new_second / (1.0 - 0.95**STEP)
    moved = master - 0.2 * first_hat / (jnp.sqrt(second_hat) + 1e-08)
    return (moved, new_moment, new_second)


def reaches(way, half, hop):
    return hop <= 3 or (hop == 4 and half == way)


def step_kernel(*refs):
    grads, state = refs[:2], (refs[2:5], refs[5:8])
    outs = (refs[8:11], refs[11:14])
    weights = refs[14:16]
    it = iter(refs[16:])
    own, par = (next(it), next(it)), (next(it), next(it))
    snd, rcv = (next(it), next(it)), (next(it), next(it))
    held = (tuple(next(it) for _ in range(3)), tuple(next(it) for _ in range(3)))
    ex_s, ex_r, sq, scale = next(it), next(it), next(it), next(it)
    own_sem, state_sem = next(it), next(it)
    par_ss, par_rs = next(it), next(it)
    rs_ss, rs_rs = next(it), next(it)
    ag_ss, ag_rs = next(it), next(it)
    cp_ss, cp_rs = next(it), next(it)
    ex_ss, ex_rs = next(it), next(it)

    dp, row, col = lax.axis_index("dp"), lax.axis_index("row"), lax.axis_index("col")
    z, core = dp // 2, dp % 2
    partner = (z * 2 + (1 - core), row, col)
    beside = (
        (lax.rem(dp + 2, 2 * NZ), row, col),
        (lax.rem(dp + 2 * NZ - 2, 2 * NZ), row, col),
    )
    peers = tuple((dp, row, lax.rem(col + j, 4)) for j in (1, 2, 3))

    def block_at(r, parity):
        return lax.rem(z + r, NZ) * 2 + parity

    def grad_block(t, r, parity):
        at = pl.multiple_of(block_at(r, parity) * 128, 128)
        if t == UP:
            return grads[t].at[0, :, pl.ds(at, 128)]
        return grads[t].at[0, pl.ds(at, 128), :]

    order = (4, 3, 5, 2, 6, 1, 7, 0)
    own_cp, par_cp = {}, {}
    for r in order:
        for t in (UP, DOWN):
            own_cp[t, r] = pltpu.make_async_copy(
                grad_block(t, r, core), own[t].at[r], own_sem.at[t, r]
            )
            own_cp[t, r].start()
    state_cp = {}
    for t in (UP, DOWN):
        for k in range(3):
            state_cp[t, k] = pltpu.make_async_copy(state[t][k], held[t][k], state_sem.at[t, k])
            state_cp[t, k].start()

    barrier = pltpu.get_barrier_semaphore()
    for device in (partner, *beside, *peers):
        pl.semaphore_signal(barrier, inc=1, device_id=device, device_id_type=MESH)
    pl.semaphore_wait(barrier, 6)

    sent = []

    def send(src, dst, ss, rs, to):
        copy = pltpu.make_async_remote_copy(
            src_ref=src, dst_ref=dst, send_sem=ss, recv_sem=rs, device_id=to, device_id_type=MESH
        )
        copy.start()
        sent.append(copy)
        return copy

    for r in order:
        for t in (UP, DOWN):
            par_cp[t, r] = send(
                grad_block(t, r, 1 - core), par[t].at[r], par_ss.at[t, r], par_rs.at[t, r], partner
            )

    def rows_of(t, half, s):
        n = PIECE[t][0]
        return pl.ds((half * S + s) * n, n)

    ready = set()

    def chip_sum(t, r, half, s):
        if (t, r) not in ready:
            ready.add((t, r))
            own_cp[t, r].wait()
            par_cp[t, r].wait_recv()
        at = rows_of(t, half, s)
        return own[t][r, at, :].astype(F32) + par[t][r, at, :].astype(F32)

    rs_cp = {}

    def reduce_hop(t, way, half, hop, s):
        total = chip_sum(t, hop if way == RIGHT else NZ - hop, half, s)
        if reaches(way, half, hop + 1):
            rs_cp[t, way, half, hop + 1, s].wait_recv()
            total += rcv[t][way, half, hop, s].astype(F32)
        snd[t][way, half, hop - 1, s] = total.astype(BF16)
        rs_cp[t, way, half, hop, s] = send(
            snd[t].at[way, half, hop - 1, s],
            rcv[t].at[way, half, hop - 1, s],
            rs_ss.at[t, way, half, hop - 1, s],
            rs_rs.at[t, way, half, hop - 1, s],
            beside[way],
        )

    def reduce_pair(t, which):
        hop, far = which
        for s in range(S):
            for way in (RIGHT, LEFT):
                reduce_hop(t, way, way if far else 1 - way, hop, s)

    ex_cp = {}

    def finish_sum(t):
        for k in range(3):
            state_cp[t, k].wait()
        acc = jnp.zeros((8, 128), F32)
        for half in (A, B):
            for s in range(S):
                base = chip_sum(t, 0, half, s)
                n = PIECE[t][0]
                for way in (RIGHT, LEFT):
                    rs_cp[t, way, half, 1, s].wait_recv()
                step = n // 2
                for i in range(0, n, step):
                    at = pl.ds((half * S + s) * n + i, step)
                    grad = own[t][0, at, :].astype(F32) + par[t][0, at, :].astype(F32)
                    for way in (RIGHT, LEFT):
                        grad += rcv[t][way, half, 0, s, pl.ds(i, step), :].astype(F32)
                    moved, mom, sec = adam_move(
                        held[t][0][at, :], held[t][1][at, :], held[t][2][at, :], grad * (1.0 / 16.0)
                    )
                    outs[t][0][at, :] = moved
                    outs[t][1][at, :] = mom
                    outs[t][2][at, :] = sec
                    square = moved * moved
                    if t == UP:
                        acc += square.reshape(step // 8, 8, 128).sum(axis=0)
                    else:
                        sq[at, :] = (
                            square[:, 0:128]
                            + square[:, 128:256]
                            + square[:, 256:384]
                            + square[:, 384:512]
                        )
        if t == DOWN:
            acc = sq[...].T.reshape(16, 8, 128).sum(axis=0)
        ex_s[t] = acc
        for j, peer in enumerate(peers):
            ex_cp[t, j] = send(ex_s.at[t], ex_r.at[t, j], ex_ss.at[t, j], ex_rs.at[t, j], peer)

    def slot(t, owner, half, s):
        n = PIECE[t][0]
        if t == UP:
            return weights[t].at[owner, rows_of(t, half, s), :]
        return weights[t].at[pl.ds(pl.multiple_of(owner * 128 + (half * S + s) * n, n), n), :]

    def renormalize(t):
        for j in range(3):
            ex_cp[t, j].wait_recv()
        total = ex_s[t] + ex_r[t, 0] + ex_r[t, 1] + ex_r[t, 2]
        factor = lax.rsqrt(total.sum(axis=0, keepdims=True) / D + 1e-06)
        rows = OPT[t][0]
        if t == UP:
            for i in range(0, rows, 64):
                norm = outs[t][0][pl.ds(i, 64), :] * factor
                outs[t][0][pl.ds(i, 64), :] = norm
                weights[t][dp, pl.ds(i, 64), :] = norm.astype(BF16)
        else:
            scale[...] = jnp.broadcast_to(factor, (128, 128)).T
            at0 = pl.multiple_of(dp * 128, 128)
            for i in range(0, rows, 16):
                f = scale[pl.ds(i, 16), :]
                norm = outs[t][0][pl.ds(i, 16), :] * jnp.concatenate([f, f, f, f], axis=1)
                outs[t][0][pl.ds(i, 16), :] = norm
                weights[t][pl.ds(pl.multiple_of(at0 + i, 16), 16), :] = norm.astype(BF16)

    ag_cp, copies = {}, []

    def to_partner(t, owner, half, s, n):
        at = slot(t, owner, half, s)
        copies.append(send(at, at, cp_ss.at[t, n, s], cp_rs.at[t, n, s], partner))

    def gather_hop(t, way, half, hop, s):
        back = NZ - (hop - 1) if way == RIGHT else hop - 1
        owner = block_at(back, core)
        at = slot(t, owner, half, s)
        if hop > 1:
            ag_cp[t, way, half, hop - 1, s].wait_recv()
        if reaches(way, half, hop):
            ag_cp[t, way, half, hop, s] = send(
                at,
                at,
                ag_ss.at[t, way, half, hop - 1, s],
                ag_rs.at[t, way, half, hop - 1, s],
                beside[way],
            )
        if hop > 1:
            n = 2 + (way * 2 + half) * 4 + hop - 2
            to_partner(t, owner, half, s, n)

    def gather_level(t, hop):
        for half in (0, 1):
            for s in range(S):
                for way in (RIGHT, LEFT):
                    h = way if half == 0 else 1 - way
                    if hop == 1 or reaches(way, h, hop - 1):
                        gather_hop(t, way, h, hop, s)
        if hop == 1:
            for half in (A, B):
                for s in range(S):
                    to_partner(t, dp, half, s, half)

    far, near = True, False
    for t, hop, side in (
        (UP, 4, far),
        (UP, 3, near),
        (DOWN, 4, far),
        (UP, 3, far),
        (UP, 2, near),
        (DOWN, 3, near),
        (UP, 2, far),
        (UP, 1, near),
        (DOWN, 3, far),
        (UP, 1, far),
        (DOWN, 2, near),
        (DOWN, 2, far),
    ):
        reduce_pair(t, (hop, side))
    finish_sum(UP)
    reduce_pair(DOWN, (1, near))
    reduce_pair(DOWN, (1, far))
    renormalize(UP)
    gather_level(UP, 1)
    finish_sum(DOWN)
    gather_level(UP, 2)
    renormalize(DOWN)
    gather_level(DOWN, 1)
    gather_level(UP, 3)
    gather_level(DOWN, 2)
    gather_level(UP, 4)
    gather_level(DOWN, 3)
    gather_level(UP, 5)
    gather_level(DOWN, 4)
    gather_level(DOWN, 5)
    for copy in copies:
        copy.wait_recv()
    for copy in sent:
        copy.wait_send()


def write_kernel(*refs):
    ins, outs, sem = refs[:8], refs[8:16], refs[16]
    copies = []
    for k in range(16):
        copies.append((ins[6].at[k], outs[6].at[:, pl.ds(k * 128, 128)]))
    copies.append((ins[7], outs[7]))
    copies += [(ins[k], outs[k]) for k in range(6)]
    copies = [pltpu.make_async_copy(a, b, sem.at[i]) for i, (a, b) in enumerate(copies)]
    for copy in copies:
        copy.start()
    for copy in copies:
        copy.wait()


def on_device(*args):
    any_space = pl.BlockSpec(memory_space=pltpu.HBM)
    vmem = pl.BlockSpec(memory_space=pltpu.VMEM)
    opt = [(shape, F32) for shape in OPT for _ in range(3)]
    mid = opt + [((2 * NZ, 512, 128), BF16), ((2048, 512), BF16)]
    out = opt + [((512, 2048), BF16), ((2048, 512), BF16)]
    dma = pltpu.SemaphoreType.DMA
    scratch = (
        [pltpu.VMEM((NZ, *BLOCK[t]), BF16) for t in (UP, DOWN)]
        + [pltpu.VMEM((NZ, *BLOCK[t]), BF16) for t in (UP, DOWN)]
        + [pltpu.VMEM((2, 2, 4, S, *PIECE[t]), BF16) for t in (UP, DOWN)]
        + [pltpu.VMEM((2, 2, 4, S, *PIECE[t]), BF16) for t in (UP, DOWN)]
        + [pltpu.VMEM(OPT[t], F32) for t in (UP, DOWN) for _ in range(3)]
        + [
            pltpu.VMEM((2, 8, 128), F32),
            pltpu.VMEM((2, 3, 8, 128), F32),
            pltpu.VMEM((128, 128), F32),
            pltpu.VMEM((128, 128), F32),
            dma((2, NZ)),
            dma((2, 3)),
            dma((2, NZ)),
            dma((2, NZ)),
            dma((2, 2, 2, 4, S)),
            dma((2, 2, 2, 4, S)),
            dma((2, 2, 2, 4, S)),
            dma((2, 2, 2, 4, S)),
            dma((2, 18, S)),
            dma((2, 18, S)),
            dma((2, 3)),
            dma((2, 3)),
        ]
    )
    mids = pl.pallas_call(
        step_kernel,
        out_shape=[pltpu.VMEM(shape, kind) for shape, kind in mid],
        in_specs=[any_space] * 8,
        out_specs=[vmem] * 8,
        scratch_shapes=scratch,
        compiler_params=pltpu.CompilerParams(
            collective_id=0, has_side_effects=True, vmem_limit_bytes=61_000_000
        ),
        name="step",
    )(*args)
    return tuple(
        pl.pallas_call(
            write_kernel,
            out_shape=[jax.ShapeDtypeStruct(shape, kind) for shape, kind in out],
            in_specs=[vmem] * 8,
            out_specs=[pl.BlockSpec(memory_space=pl.ANY)] * 8,
            scratch_shapes=[dma((23,))],
            compiler_params=pltpu.CompilerParams(vmem_limit_bytes=20 * 2**20),
            name="write",
        )(*mids)
    )


def solution(mesh):
    up, down = P("col", ("row", "dp")), P(("row", "dp"), "col")
    return jax.shard_map(
        on_device,
        mesh=mesh,
        in_specs=(P("dp", "col", "row"), P("dp", "row", "col"), up, up, up, down, down, down),
        out_specs=(up, up, up, down, down, down, P("col", "row"), P("row", "col")),
        check_vma=False,
    )
```

```python
import jax
import jax.numpy as jnp
from jax import lax
from jax.experimental import pallas as pl
from jax.experimental.pallas import tpu as pltpu
from jax.sharding import PartitionSpec as P

D = 2048
STEP = 10
MESH = pl.DeviceIdType.MESH
F32, BF16 = jnp.float32, jnp.bfloat16
NZ = 8
S = 2
REDUCE, FINISH, NORM, GATHER = 0, 1, 2, 3
ORDER = (
    (0, 0, 4, 1, 0),
    (0, 0, 4, 1, 1),
    (0, 0, 3, 0, 0),
    (0, 0, 3, 0, 1),
    (0, 1, 4, 1, 0),
    (0, 1, 4, 1, 1),
    (0, 0, 3, 1, 0),
    (0, 0, 3, 1, 1),
    (0, 0, 2, 0, 0),
    (0, 0, 2, 0, 1),
    (0, 1, 3, 0, 0),
    (0, 1, 3, 0, 1),
    (0, 0, 2, 1, 0),
    (0, 0, 2, 1, 1),
    (0, 0, 1, 0, 0),
    (0, 0, 1, 0, 1),
    (0, 1, 3, 1, 0),
    (0, 1, 3, 1, 1),
    (0, 0, 1, 1, 0),
    (0, 0, 1, 1, 1),
    (0, 1, 2, 0, 0),
    (0, 1, 2, 0, 1),
    (0, 1, 2, 1, 0),
    (0, 1, 2, 1, 1),
    (1, 0, 0, 0, 0),
    (0, 1, 1, 0, 0),
    (0, 1, 1, 0, 1),
    (0, 1, 1, 1, 0),
    (0, 1, 1, 1, 1),
    (2, 0, 0, 0, 0),
    (3, 0, 1, 1, 0),
    (3, 0, 1, 1, 1),
    (3, 0, 1, 0, 0),
    (3, 0, 1, 0, 1),
    (1, 1, 0, 0, 0),
    (3, 0, 2, 1, 0),
    (3, 0, 2, 1, 1),
    (3, 0, 2, 0, 0),
    (3, 0, 2, 0, 1),
    (2, 1, 0, 0, 0),
    (3, 1, 1, 1, 0),
    (3, 1, 1, 1, 1),
    (3, 1, 1, 0, 0),
    (3, 1, 1, 0, 1),
    (3, 0, 3, 1, 0),
    (3, 0, 3, 1, 1),
    (3, 0, 3, 0, 0),
    (3, 0, 3, 0, 1),
    (3, 1, 2, 1, 0),
    (3, 1, 2, 1, 1),
    (3, 1, 2, 0, 0),
    (3, 1, 2, 0, 1),
    (3, 0, 4, 1, 0),
    (3, 0, 4, 1, 1),
    (3, 0, 4, 0, 0),
    (3, 0, 4, 0, 1),
    (3, 1, 3, 1, 0),
    (3, 1, 3, 1, 1),
    (3, 1, 3, 0, 0),
    (3, 1, 3, 0, 1),
    (3, 0, 5, 1, 0),
    (3, 0, 5, 1, 1),
    (3, 1, 4, 1, 0),
    (3, 1, 4, 1, 1),
    (3, 1, 4, 0, 0),
    (3, 1, 4, 0, 1),
    (3, 1, 5, 1, 0),
    (3, 1, 5, 1, 1),
)
SEMS = [
    pltpu.SemaphoreType.DMA(shape)
    for shape in ((2, NZ), (2, NZ), (2, 3), (2, NZ), (2, 14, S), (2, 14, S)) + ((2,),) * 7
]
UP, DOWN = 0, 1
RIGHT, LEFT = 0, 1
A, B = 0, 1
BLOCK = ((512, 128), (128, 512))
PIECE = tuple((r // (2 * S), c) for r, c in BLOCK)
OPT = ((512, 128), (128, 512))


def adam_move(master, moment, second, grad):
    new_moment = 0.9 * moment + 0.1 * grad
    new_second = 0.95 * second + 0.05 * grad * grad
    first_hat = new_moment / (1.0 - 0.9**STEP)
    second_hat = new_second / (1.0 - 0.95**STEP)
    moved = master - 0.2 * first_hat / (jnp.sqrt(second_hat) + 1e-08)
    return (moved, new_moment, new_second)


def unit(way, half, hop):
    return way * 7 + (hop - 1) * 2 + (half if hop <= 3 else 0)


def reaches(way, half, hop):
    return hop <= 3 or (hop == 4 and half == way)


def step_kernel(*refs):
    def scoped(*sems):
        step_body(*refs, *sems)

    pl.run_scoped(scoped, *SEMS)


def step_body(*refs):
    grads, state = refs[:2], (refs[2:5], refs[5:8])
    outs = (refs[8:11], refs[11:14])
    weights = refs[14:16]
    it = iter(refs[16:])
    own, away, par = tuple((next(it), next(it)) for _ in range(3))
    snd, rcv = (next(it), next(it)), (next(it), next(it))
    held = next(it), next(it)
    ex_s, ex_r, sq, scale = next(it), next(it), next(it), next(it)
    own_sem, away_sem, state_sem = next(it), next(it), next(it)
    par_rs, rs_rs, ag_rs = next(it), next(it), next(it)
    cp_rs, ex_rs = next(it), next(it)
    par_ss, rs_ss, ag_ss, cp_ss, ex_ss = tuple(next(it) for _ in range(5))

    dp, row, col = lax.axis_index("dp"), lax.axis_index("row"), lax.axis_index("col")
    z, core = dp // 2, dp % 2
    partner = (z * 2 + (1 - core), row, col)
    beside = (
        (lax.rem(dp + 2, 2 * NZ), row, col),
        (lax.rem(dp + 2 * NZ - 2, 2 * NZ), row, col),
    )
    peers = tuple((dp, row, lax.rem(col + j, 4)) for j in (1, 2, 3))

    def block_at(r, parity):
        return lax.rem(z + r, NZ) * 2 + parity

    def grad_block(t, r, parity):
        at = pl.multiple_of(block_at(r, parity) * 128, 128)
        if t == UP:
            return grads[t].at[0, :, pl.ds(at, 128)]
        return grads[t].at[0, pl.ds(at, 128), :]

    barrier = pltpu.get_barrier_semaphore()
    for device in (partner, *beside, *peers):
        pl.semaphore_signal(barrier, inc=1, device_id=device, device_id_type=MESH)

    order = (4, 3, 5, 2, 6, 1, 7, 0)
    own_cp, away_cp, par_cp = {}, {}, {}
    for r in order:
        for t in (UP, DOWN):
            away_cp[t, r] = pltpu.make_async_copy(
                grad_block(t, r, 1 - core), away[t].at[r], away_sem.at[t, r]
            )
            away_cp[t, r].start()
            own_cp[t, r] = pltpu.make_async_copy(
                grad_block(t, r, core), own[t].at[r], own_sem.at[t, r]
            )
            own_cp[t, r].start()
    state_cp = {}
    for t in (UP, DOWN):
        for k in range(3):
            state_cp[t, k] = pltpu.make_async_copy(state[t][k], held[t].at[k], state_sem.at[t, k])
            state_cp[t, k].start()

    def send(src, dst, ss, rs, to):
        copy = pltpu.make_async_remote_copy(
            src_ref=src, dst_ref=dst, send_sem=ss, recv_sem=rs, device_id=to, device_id_type=MESH
        )
        copy.start()
        return copy

    def took(ref, sem):
        pltpu.make_async_copy(ref, ref, sem).wait()

    pl.semaphore_wait(barrier, 6)
    for r in order:
        for t in (UP, DOWN):
            away_cp[t, r].wait()
            par_cp[t, r] = send(
                away[t].at[r], par[t].at[r], par_ss.at[t], par_rs.at[t, r], partner
            )

    def rows_of(t, half, s):
        n = PIECE[t][0]
        return pl.ds((half * S + s) * n, n)

    ready = set()

    def chip_sum(t, r, half, s):
        if (t, r) not in ready:
            ready.add((t, r))
            own_cp[t, r].wait()
            par_cp[t, r].wait_recv()
        at = rows_of(t, half, s)
        return own[t][r, at, :].astype(F32) + par[t][r, at, :].astype(F32)

    rs_cp = {}

    def reduce_hop(t, way, half, hop, s):
        total = chip_sum(t, hop if way == RIGHT else NZ - hop, half, s)
        if reaches(way, half, hop + 1):
            rs_cp[t, way, half, hop + 1, s].wait_recv()
            total += rcv[t][unit(way, half, hop + 1), s].astype(F32)
        u = unit(way, half, hop)
        snd[t][u, s] = total.astype(BF16)
        rs_cp[t, way, half, hop, s] = send(
            snd[t].at[u, s], rcv[t].at[u, s], rs_ss.at[t], rs_rs.at[t, u, s], beside[way]
        )

    def finish_sum(t):
        for k in range(3):
            state_cp[t, k].wait()
        acc = jnp.zeros((8, 128), F32)
        for half in (A, B):
            for s in range(S):
                base = chip_sum(t, 0, half, s)
                n = PIECE[t][0]
                for way in (RIGHT, LEFT):
                    rs_cp[t, way, half, 1, s].wait_recv()
                step = n // 2
                for i in range(0, n, step):
                    at = pl.ds((half * S + s) * n + i, step)
                    grad = own[t][0, at, :].astype(F32) + par[t][0, at, :].astype(F32)
                    for way in (RIGHT, LEFT):
                        u = unit(way, half, 1)
                        grad += rcv[t][u, s, pl.ds(i, step), :].astype(F32)
                    moved, mom, sec = adam_move(
                        held[t][0, at, :], held[t][1, at, :], held[t][2, at, :], grad * (1.0 / 16.0)
                    )
                    outs[t][0][at, :] = moved
                    outs[t][1][at, :] = mom
                    outs[t][2][at, :] = sec
                    square = moved * moved
                    if t == UP:
                        acc += square.reshape(step // 8, 8, 128).sum(axis=0)
                    else:
                        sq[at, :] = (
                            square[:, 0:128]
                            + square[:, 128:256]
                            + square[:, 256:384]
                            + square[:, 384:512]
                        )
        if t == DOWN:
            acc = sq[...].T.reshape(16, 8, 128).sum(axis=0)
        ex_s[t] = acc
        for j, peer in enumerate(peers):
            send(ex_s.at[t], ex_r.at[t, j], ex_ss.at[t], ex_rs.at[t], peer)

    def slot(t, owner, half, s):
        n = PIECE[t][0]
        if t == UP:
            return weights[t].at[owner, rows_of(t, half, s), :]
        return weights[t].at[pl.ds(pl.multiple_of(owner * 128 + (half * S + s) * n, n), n), :]

    def renormalize(t):
        took(ex_r.at[t], ex_rs.at[t])
        total = ex_s[t] + ex_r[t, 0] + ex_r[t, 1] + ex_r[t, 2]
        factor = lax.rsqrt(total.sum(axis=0, keepdims=True) / D + 1e-06)
        rows = OPT[t][0]
        if t == UP:
            for i in range(0, rows, 64):
                norm = outs[t][0][pl.ds(i, 64), :] * factor
                outs[t][0][pl.ds(i, 64), :] = norm
                weights[t][dp, pl.ds(i, 64), :] = norm.astype(BF16)
        else:
            scale[...] = jnp.broadcast_to(factor, (128, 128)).T
            at0 = pl.multiple_of(dp * 128, 128)
            for i in range(0, rows, 16):
                f = scale[pl.ds(i, 16), :]
                norm = outs[t][0][pl.ds(i, 16), :] * jnp.concatenate([f, f, f, f], axis=1)
                outs[t][0][pl.ds(i, 16), :] = norm
                weights[t][pl.ds(pl.multiple_of(at0 + i, 16), 16), :] = norm.astype(BF16)

    ag_cp = {}

    def to_partner(t, owner, half, s):
        at = slot(t, owner, half, s)
        send(at, at, cp_ss.at[t], cp_rs.at[t], partner)

    def gather_hop(t, way, half, hop, s):
        back = NZ - (hop - 1) if way == RIGHT else hop - 1
        owner = block_at(back, core)
        at = slot(t, owner, half, s)
        if hop > 1:
            ag_cp[t, way, half, hop - 1, s].wait_recv()
        if reaches(way, half, hop):
            ag_cp[t, way, half, hop, s] = send(
                at,
                at,
                ag_ss.at[t],
                ag_rs.at[t, unit(way, half, hop), s],
                beside[way],
            )
        if hop > 1:
            to_partner(t, owner, half, s)

    for kind, t, hop, far, s in ORDER:
        if kind == REDUCE:
            for way in (RIGHT, LEFT):
                reduce_hop(t, way, way if far else 1 - way, hop, s)
        elif kind == FINISH:
            finish_sum(t)
        elif kind == NORM:
            renormalize(t)
        else:
            for way in (RIGHT, LEFT):
                gather_hop(t, way, way if far else 1 - way, hop, s)
            if hop == 1 and far:
                for half in (A, B):
                    to_partner(t, dp, half, s)

    for t in (UP, DOWN):
        part = 1 if t == UP else BLOCK[t][0]
        took(weights[t].at[pl.ds(0, 8 * part)], cp_rs.at[t])
        took(weights[t].at[pl.ds(0, 8 * part)], cp_ss.at[t])
        took(weights[t].at[pl.ds(0, 7 * part)], ag_ss.at[t])
        took(snd[t], rs_ss.at[t])
        took(par[t], par_ss.at[t])
        took(ex_r.at[t], ex_ss.at[t])


def write_kernel(*refs):
    ins, outs, sem = refs[:8], refs[8:16], refs[16]
    copies = []
    for k in range(16):
        copies.append((ins[6].at[k], outs[6].at[:, pl.ds(k * 128, 128)]))
    copies.append((ins[7], outs[7]))
    copies += [(ins[k], outs[k]) for k in range(6)]
    copies = [pltpu.make_async_copy(a, b, sem.at[i]) for i, (a, b) in enumerate(copies)]
    for copy in copies:
        copy.start()
    for copy in copies:
        copy.wait()


def on_device(*args):
    any_space = pl.BlockSpec(memory_space=pltpu.HBM)
    vmem = pl.BlockSpec(memory_space=pltpu.VMEM)
    opt = [(shape, F32) for shape in OPT for _ in range(3)]
    mid = opt + [((2 * NZ, 512, 128), BF16), ((2048, 512), BF16)]
    out = opt + [((512, 2048), BF16), ((2048, 512), BF16)]
    dma = pltpu.SemaphoreType.DMA
    both = (UP, DOWN)
    scratch = (
        [pltpu.VMEM((NZ, *BLOCK[t]), BF16) for _ in range(3) for t in both]
        + [pltpu.VMEM((14, S, *PIECE[t]), BF16) for _ in range(2) for t in both]
        + [pltpu.VMEM((3, *OPT[t]), F32) for t in both]
        + [
            pltpu.VMEM((2, 8, 128), F32),
            pltpu.VMEM((2, 3, 8, 128), F32),
            pltpu.VMEM((128, 128), F32),
            pltpu.VMEM((128, 128), F32),
        ]
    )
    mids = pl.pallas_call(
        step_kernel,
        out_shape=[pltpu.VMEM(shape, kind) for shape, kind in mid],
        in_specs=[any_space] * 8,
        out_specs=[vmem] * 8,
        scratch_shapes=scratch,
        compiler_params=pltpu.CompilerParams(
            collective_id=0, has_side_effects=True, vmem_limit_bytes=61_000_000
        ),
        name="step",
    )(*args)
    return tuple(
        pl.pallas_call(
            write_kernel,
            out_shape=[jax.ShapeDtypeStruct(shape, kind) for shape, kind in out],
            in_specs=[vmem] * 8,
            out_specs=[pl.BlockSpec(memory_space=pl.ANY)] * 8,
            scratch_shapes=[dma((23,))],
            compiler_params=pltpu.CompilerParams(vmem_limit_bytes=20 * 2**20),
            name="write",
        )(*mids)
    )


def solution(mesh):
    up, down = P("col", ("row", "dp")), P(("row", "dp"), "col")
    return jax.shard_map(
        on_device,
        mesh=mesh,
        in_specs=(P("dp", "col", "row"), P("dp", "row", "col"), up, up, up, down, down, down),
        out_specs=(up, up, up, down, down, down, P("col", "row"), P("row", "col")),
        check_vma=False,
    )
```
